32 devices in a mesh: dp: 8 (over z, x), cand: 4 (over y, core).
Axes of the slice: x: 2, y: 2, z: 4, core: 2. Of those that a mesh axis runs over, the one named last changes fastest.
Arguments:
- hidden: bfloat16 [16, 32, 128, 768], P('dp', 'cand'), may hold values from -24 to 24
- attn_weight: bfloat16 [768, 3072], P('dp'), may hold values from -1 to 1
- norm_gain: float32 [768], replicated, may hold values from 0.2 to 4
- pos_bias: float32 [12, 128, 128], replicated, may hold values from -5 to 5
- score_weight: float32 [768], replicated, may hold values from -4 to 4
- pair_lengths: int32 [16, 32], P('dp', 'cand'), may hold values from 32 to 128
- labels: int32 [16, 32], P('dp', 'cand'), may hold values from 0 to 3
Outputs:
- update: float32 [768, 3072], P('dp')
- loss: float32 [16], P('dp')
The draws below stay inside these ranges and needn't reach their ends.
All inputs are finite; a program needn't handle non-finite values.
Results may differ from the reference program's by a relative error of at most 0.017.
Values may be sent and summed in bfloat16 or wider, within the bound.
No kernel may reach another device: no remote copies, remote signals or barrier semaphores. Data moves between devices by JAX's collectives and lax.ppermute only.
A program may use at most 128 MiB of HBM per device.

```python
import jax
import jax.numpy as jnp
from jax import lax

D = 768
HEADS = 12
HEAD = 64
SEQ = 128
CANDS = 32
QUERIES = 16


def draw_norm_gain(key, part):
    place = jnp.arange(D, dtype=jnp.int32).astype(jnp.float32) / jnp.float32(D)
    jitter = jax.random.uniform(jax.random.fold_in(key, 7401), (D,), jnp.float32, 0.75, 1.25)
    lowest, highest = (0.4, 2.0)
    values = jnp.exp(jnp.log(lowest) + (jnp.log(highest) - jnp.log(lowest)) * place) * jitter
    return jnp.clip(values, 0.2, 4.0)


def draw_score_weight(key, part):
    values = jax.random.normal(jax.random.fold_in(key, 7102), (D,), jnp.float32)
    values = jnp.clip(values, -6.0, 6.0) * jnp.sqrt(4.0 / jnp.float32(D))
    return jnp.clip(values, -4.0, 4.0)


def draw_attn_weight(key, part):
    values = jax.random.normal(jax.random.fold_in(key, 7301), (D, 4 * D), jnp.float32)
    values = jnp.clip(values, -6.0, 6.0) / jnp.sqrt(jnp.float32(D))
    column = jnp.arange(4 * D, dtype=jnp.int32)
    factor = jnp.where(column < D, 1.0 / jnp.sqrt(jnp.float32(HEAD)), 1.0)
    values = jnp.clip(values * factor[None, :], -1.0, 1.0)
    return values.astype(jnp.bfloat16)


def draw_hidden(key, part):
    normal_part = jax.random.normal(jax.random.fold_in(key, 7201), (QUERIES, CANDS, SEQ, D), jnp.float32)
    normal_part = jnp.clip(normal_part, -6.0, 6.0)
    values = normal_part
    return jnp.clip(values, -24.0, 24.0).astype(jnp.bfloat16)


def touch_ends(drawn, rng, least, largest):
    extent = drawn.shape
    index_at = [jax.random.randint(jax.random.fold_in(rng, axis), (), 0, extent[axis]) for axis in range(len(extent))]
    drawn = drawn.at[tuple(index_at)].set(least)
    longest = extent.index(max(extent))
    index_at[longest] = (index_at[longest] + 1) % extent[longest]
    return drawn.at[tuple(index_at)].set(largest)


def gaussian(stream_key, dims, scale, bound, kind=jnp.bfloat16):
    entries = jax.random.normal(stream_key, dims, jnp.float32) * scale
    return jnp.minimum(jnp.maximum(entries, -bound), bound).astype(kind)


def setup_inputs(seed: int = 0) -> dict:
    key_list = jax.random.split(jax.random.key(seed), 8)
    return {
        "hidden": draw_hidden(jax.random.fold_in(key_list[7], 71), 0),
        "attn_weight": draw_attn_weight(jax.random.fold_in(key_list[7], 71), 0),
        "norm_gain": draw_norm_gain(jax.random.fold_in(key_list[7], 71), 0),
        "pos_bias": gaussian(key_list[3], (HEADS, SEQ, SEQ), 1.0, 5.0, jnp.float32),
        "score_weight": draw_score_weight(jax.random.fold_in(key_list[7], 71), 0),
        "pair_lengths": touch_ends(jax.random.randint(key_list[5], (QUERIES, CANDS), SEQ // 4, SEQ + 1), jax.random.fold_in(key_list[5], 1), SEQ // 4, SEQ).astype(jnp.int32),
        "labels": touch_ends(jax.random.randint(key_list[6], (QUERIES, CANDS), 0, 4), jax.random.fold_in(key_list[6], 1), 0, 3).astype(jnp.int32),
    }


EPS = 1e-06

def rms_rows(values, gain):
    factor = lax.rsqrt(lax.optimization_barrier(jnp.mean(values * values, axis=-1, keepdims=True)) + EPS)
    return values * factor * gain

def attend(qkv, pos_bias, pair_len):
    batch, seq, triple = qkv.shape
    width = triple // 3
    heads = pos_bias.shape[0]
    head_size = width // heads
    parts = qkv.reshape(batch, seq, 3, heads, head_size).astype(jnp.float32)
    logits = jnp.einsum('bqhd,bkhd->bhqk', parts[:, :, 0], parts[:, :, 1])
    logits = logits + pos_bias[None]
    valid = jnp.arange(seq, dtype=jnp.int32)[None, :] < pair_len[:, None]
    logits = jnp.where(valid[:, None, None, :], logits, -1e+30)
    highest = lax.optimization_barrier(jnp.max(logits, axis=-1, keepdims=True))
    expo = jnp.exp(logits - highest)
    probs = (expo / lax.optimization_barrier(jnp.sum(expo, axis=-1, keepdims=True))).astype(jnp.bfloat16)
    context = jnp.einsum('bhqk,bkhd->bqhd', probs.astype(jnp.float32), parts[:, :, 2])
    return context.astype(jnp.bfloat16).reshape(batch, seq, width)

def forward(tokens, weights, norm_gain, pos_bias, pair_len):
    batch, seq, width = tokens.shape
    values = tokens.astype(jnp.float32)
    normed = rms_rows(values, norm_gain).astype(jnp.bfloat16)
    qkv = jnp.dot(normed.reshape(-1, width), weights[:, :3 * width], preferred_element_type=jnp.float32)
    qkv = qkv.astype(jnp.bfloat16).reshape(batch, seq, 3 * width)
    context = attend(qkv, pos_bias, pair_len)
    out_rows = values + jnp.dot(context.reshape(-1, width), weights[:, 3 * width:], preferred_element_type=jnp.float32).reshape(batch, seq, width)
    live = (jnp.arange(seq, dtype=jnp.int32)[None, :] < pair_len[:, None]).astype(jnp.float32)
    share = live / pair_len.astype(jnp.float32)[:, None]
    pooled = lax.optimization_barrier(jnp.sum(out_rows * share[:, :, None], axis=1))
    return (normed, qkv, context, pooled, share)

def score_head(pooled, score_weight):
    return lax.optimization_barrier(jnp.sum(rms_rows(pooled, 1.0) * score_weight, axis=-1))

def backward(normed, qkv, context, pooled, share, weights, pos_bias, pair_len, score_weight, score_grad):
    batch, seq, width = normed.shape
    unused, head_back = jax.vjp(lambda vector: score_head(vector, score_weight), pooled)
    pooled_grad = head_back(score_grad)[0]
    out_grad = (pooled_grad[:, None, :] * share[:, :, None]).astype(jnp.bfloat16)
    flat_out = out_grad.reshape(-1, width)
    context_grad = jnp.dot(flat_out, weights[:, 3 * width:].T, preferred_element_type=jnp.float32)
    context_grad = context_grad.astype(jnp.bfloat16).reshape(batch, seq, width)
    unused2, attend_back = jax.vjp(lambda block: attend(block, pos_bias, pair_len), qkv)
    qkv_grad = attend_back(context_grad)[0].reshape(-1, 3 * width)
    first = jnp.dot(normed.reshape(-1, width).T, qkv_grad, preferred_element_type=jnp.float32)
    second = jnp.dot(context.reshape(-1, width).T, flat_out, preferred_element_type=jnp.float32)
    return jnp.concatenate([first, second], axis=1)

def reference(hidden, attn_weight, norm_gain, pos_bias, score_weight, pair_lengths, labels):
    width = hidden.shape[3]

    def scores_of(pair):
        tokens, pair_len = pair
        unused_a, unused_b, unused_c, pooled, unused_d = forward(tokens, attn_weight, norm_gain, pos_bias, pair_len)
        return score_head(pooled, score_weight)
    scores = lax.map(scores_of, (hidden, pair_lengths))
    highest = lax.optimization_barrier(jnp.max(scores, axis=1, keepdims=True))
    expsum = lax.optimization_barrier(jnp.sum(jnp.exp(scores - highest), axis=1, keepdims=True))
    target = jnp.exp(labels.astype(jnp.float32))
    target_sum = lax.optimization_barrier(jnp.sum(target, axis=1, keepdims=True))
    target_dot = lax.optimization_barrier(jnp.sum(target * scores, axis=1, keepdims=True))
    loss = (highest + jnp.log(expsum) - target_dot / target_sum)[:, 0]
    score_grad = jnp.exp(scores - highest) / expsum - target / target_sum

    def accumulate(total, pair):
        tokens, pair_len, grad_row = pair
        normed, qkv, context, pooled, share = forward(tokens, attn_weight, norm_gain, pos_bias, pair_len)
        term = backward(normed, qkv, context, pooled, share, attn_weight, pos_bias, pair_len, score_weight, grad_row)
        return (total + term, None)
    start = jnp.zeros((width, 4 * width), jnp.float32)
    grad, unused = lax.scan(accumulate, start, (hidden, pair_lengths, score_grad))
    rms_value = jnp.sqrt(jnp.sum(grad * grad) / (4.0 * width * width))
    update = grad / (rms_value + EPS)
    return (update, loss)
```

```python
import functools

import jax
import jax.numpy as jnp
from jax import lax
from jax.experimental import pallas as pl
from jax.experimental.pallas import tpu as pltpu
from jax.sharding import PartitionSpec as P

EPS = 1e-06
F32 = jnp.float32
BF16 = jnp.bfloat16
LANES = 128
NN = (((1,), (0,)), ((), ()))
NT = (((1,), (1,)), ((), ()))
TN = (((0,), (0,)), ((), ()))


def dot(a, b, dims=NN):
    return lax.dot_general(a, b, dims, preferred_element_type=F32)


def split2(x):
    high = x.astype(BF16)
    return high, (x - high.astype(F32)).astype(BF16)


def norm_kernel(step, len_ref, hid_ref, gain_ref, normed_ref, normed_t_ref, mean_ref):
    seq = hid_ref.shape[1]
    for b in range(step):
        pair_len = len_ref[pl.program_id(0) * step + b]
        x = hid_ref[b].astype(F32)
        factor = lax.rsqrt(jnp.mean(x * x, axis=-1, keepdims=True) + EPS)
        n = (x * factor * gain_ref[...]).astype(BF16)
        normed_ref[b * seq : (b + 1) * seq, :] = n
        normed_t_ref[:, b * seq : (b + 1) * seq] = n.T
        live = lax.broadcasted_iota(jnp.int32, x.shape, 0) < pair_len
        total = jnp.sum(jnp.where(live, x, 0.0), axis=0, keepdims=True)
        mean_ref[b] = total / pair_len.astype(F32)


def fwd_kernel(step, heads, len_ref, normed_ref, w_ref, bias_ref, qkv_ref, pt_ref, c_ref, ctx_ref):
    seq = bias_ref.shape[1]
    width = w_ref.shape[1] // 3
    hd = width // heads
    qkv_ref[...] = dot(normed_ref[...], w_ref[...]).astype(BF16)
    ones = jnp.ones((8, seq), BF16)
    for b in range(step):
        pair_len = len_ref[pl.program_id(0) * step + b]
        rows = slice(b * seq, (b + 1) * seq)
        key_live = lax.broadcasted_iota(jnp.int32, (seq, seq), 0) < pair_len
        query_live = lax.broadcasted_iota(jnp.int32, (1, seq), 1) < pair_len
        sums = []
        for h in range(heads):
            q = qkv_ref[rows, h * hd : (h + 1) * hd]
            k = qkv_ref[rows, width + h * hd : width + (h + 1) * hd]
            st = dot(k, q, NT) + bias_ref[h]
            st = jnp.where(key_live, st, -1e30)
            e = jnp.exp(st - jnp.max(st, axis=0, keepdims=True))
            share = jnp.where(query_live, 1.0 / jnp.sum(e, axis=0, keepdims=True), 0.0)
            pt = (e * share).astype(BF16)
            pt_ref[b, h] = pt
            sums.append(dot(ones, pt, NT)[0:1, :])
        c = jnp.concatenate(sums, axis=0)
        c_ref[b] = c
        high, low = split2(c)
        v = qkv_ref[rows, 2 * width : 3 * width]
        ctx = dot(high, v) + dot(low, v)
        col_head = lax.broadcasted_iota(jnp.int32, ctx.shape, 1) // hd
        own = col_head == lax.broadcasted_iota(jnp.int32, ctx.shape, 0)
        ctx_ref[b] = jnp.sum(jnp.where(own, ctx, 0.0), axis=0, keepdims=True)


def value_kernel(groups, heads, *refs):
    c_refs, (normed_ref, a_ref) = refs[:groups], refs[groups:]
    normed = normed_ref[...]
    for g in range(groups):
        a_ref[0, g * heads : (g + 1) * heads, :] = dot(c_refs[g][0].astype(BF16), normed)


def score_kernel(groups, *refs):
    ctx_refs = refs[:groups]
    mean_ref, len_ref, label_ref, wo_ref, sw_ref, pooled_ref, ctx_ref, out_ref = refs[groups:]
    ctx = jnp.concatenate([r[...] for r in ctx_refs], axis=1)
    ctx_ref[...] = ctx
    high, low = split2(ctx / len_ref[...])
    pooled = mean_ref[...] + dot(high, wo_ref[...]) + dot(low, wo_ref[...])
    pooled_ref[...] = pooled
    factor = lax.rsqrt(jnp.mean(pooled * pooled, axis=-1, keepdims=True) + EPS)
    scores = jnp.sum(pooled * factor * sw_ref[...], axis=-1, keepdims=True)
    lane = lax.broadcasted_iota(jnp.int32, out_ref.shape, 1)
    out_ref[...] = jnp.where(lane == 0, scores, label_ref[...])


def head_kernel(c_local, heads, all_ref, pooled_ref, ctx_ref, len_ref, a_ref, wo_ref, sw_ref,
                g_ref, dwo_ref, dwv_ref, loss_ref):
    pairs, width = pooled_ref.shape
    hd = width // heads
    every = all_ref[...]
    score, label = every[:, 0:1], every[:, 1:2]
    own_score, own_label = every[:pairs, 0:1], every[:pairs, 1:2]
    weight = jnp.exp(label)
    query = lax.rem(lax.broadcasted_iota(jnp.int32, score.shape, 0), pairs) // c_local
    own_query = lax.broadcasted_iota(jnp.int32, own_score.shape, 0) // c_local
    score_grad = jnp.zeros_like(own_score)
    lane = lax.broadcasted_iota(jnp.int32, loss_ref.shape, 1)
    losses = jnp.zeros(loss_ref.shape, F32)
    for q in range(pairs // c_local):
        mine = query == q
        highest = jnp.max(jnp.where(mine, score, -jnp.inf), axis=0, keepdims=True)
        expsum = jnp.sum(jnp.where(mine, jnp.exp(score - highest), 0.0), axis=0, keepdims=True)
        tsum = jnp.sum(jnp.where(mine, weight, 0.0), axis=0, keepdims=True)
        tdot = jnp.sum(jnp.where(mine, weight * score, 0.0), axis=0, keepdims=True)
        losses = jnp.where(lane == q, highest + jnp.log(expsum) - tdot / tsum, losses)
        grad = jnp.exp(own_score - highest) / expsum - jnp.exp(own_label) / tsum
        score_grad = jnp.where(own_query == q, grad, score_grad)
    loss_ref[...] = losses
    pooled = pooled_ref[...]
    sw = sw_ref[...]
    factor = lax.rsqrt(jnp.mean(pooled * pooled, axis=-1, keepdims=True) + EPS)
    inner = jnp.sum(pooled * sw, axis=-1, keepdims=True) / width
    pooled_grad = score_grad * (factor * sw - pooled * (factor * factor * factor * inner))
    out_grad = (pooled_grad / len_ref[...]).astype(BF16)
    g = dot(out_grad, wo_ref[...], NT).astype(BF16)
    g_ref[...] = g
    high, low = split2(ctx_ref[...])
    dwo_ref[...] = dot(
        jnp.concatenate([high, low], axis=0), jnp.concatenate([out_grad, out_grad], axis=0), TN
    ).astype(BF16)
    col_head = lax.broadcasted_iota(jnp.int32, g.shape, 1) // hd
    g32 = g.astype(F32)
    spread = [jnp.where(col_head == h, g32, 0.0) for h in range(heads)]
    dwv_ref[...] = dot(
        a_ref[...].astype(BF16), jnp.concatenate(spread, axis=0).astype(BF16), TN
    ).astype(BF16)


def bwd_kernel(step, heads, qkv_ref, pt_ref, g_ref, nt_ref, out_ref, acc_ref, dqt_ref, dk_ref):
    seq = pt_ref.shape[2]
    width = qkv_ref.shape[1] // 3
    hd = width // heads
    for b in range(step):
        rows = slice(b * seq, (b + 1) * seq)
        kt = qkv_ref[rows, width : 2 * width].T
        for h in range(heads):
            cols = slice(h * hd, (h + 1) * hd)
            v = qkv_ref[rows, 2 * width + h * hd : 2 * width + (h + 1) * hd]
            u = dot(v, jnp.broadcast_to(g_ref[b, 0:1, cols], (seq, hd)), NT)
            pt = pt_ref[b, h].astype(F32)
            r = jnp.sum(pt * u, axis=0, keepdims=True)
            t = (pt * (u - r)).astype(BF16)
            dk_ref[rows, cols] = dot(t, qkv_ref[rows, cols]).astype(BF16)
            dqt_ref[cols, rows] = dot(kt[cols, :], t).astype(BF16)

    @pl.when(pl.program_id(0) == 0)
    def _():
        acc_ref[...] = jnp.zeros_like(acc_ref)

    acc_ref[:, :width] += dot(nt_ref[...], dqt_ref[...], NT)
    acc_ref[:, width:] += dot(nt_ref[...], dk_ref[...])

    @pl.when(pl.program_id(0) == pl.num_programs(0) - 1)
    def _():
        out_ref[...] = acc_ref[...].astype(BF16)


VM = pl.BlockSpec(memory_space=pltpu.VMEM)


def struct(shape, dtype):
    return jax.ShapeDtypeStruct(shape, dtype)


def shards(hidden, attn_weight, norm_gain, pos_bias, score_weight, pair_lengths, labels):
    q_local, c_local, seq, width = hidden.shape
    heads = pos_bias.shape[0]
    hd = width // heads
    pairs = q_local * c_local
    group = max(1, min(heads, 256 // hd))
    while heads % group:
        group -= 1
    groups = heads // group
    gw = group * hd
    step = 4
    while pairs % step:
        step //= 2
    grid = pairs // step
    tokens = hidden.reshape(pairs, seq, width)
    lens = pair_lengths.reshape(-1)
    len_col = lens.astype(F32)[:, None]
    label_col = labels.reshape(-1).astype(F32)[:, None]
    bias_t = jnp.swapaxes(pos_bias, 1, 2)
    sw = score_weight[None, :]

    weights = lax.all_gather(attn_weight, "dp", axis=0, tiled=True)
    chunks = [
        jnp.concatenate(
            [weights[:, s * width + g * gw : s * width + (g + 1) * gw] for s in range(3)], axis=1
        )
        for g in range(groups)
    ]
    wo = weights[:, 3 * width :]

    normed, normed_t, mean = pl.pallas_call(
        functools.partial(norm_kernel, step),
        grid_spec=pltpu.PrefetchScalarGridSpec(
            num_scalar_prefetch=1,
            grid=(grid,),
            in_specs=[
                pl.BlockSpec((step, seq, width), lambda i, s: (i, 0, 0)),
                pl.BlockSpec((1, width), lambda i, s: (0, 0)),
            ],
            out_specs=[
                pl.BlockSpec((step * seq, width), lambda i, s: (i, 0)),
                pl.BlockSpec((width, step * seq), lambda i, s: (0, i)),
                pl.BlockSpec((step, 1, width), lambda i, s: (i, 0, 0)),
            ],
        ),
        out_shape=[
            struct((pairs * seq, width), BF16),
            struct((width, pairs * seq), BF16),
            struct((pairs, 1, width), F32),
        ],
        name="norm",
    )(lens, tokens, norm_gain[None, :])

    saved = []
    for g in range(groups):
        saved.append(
            pl.pallas_call(
                functools.partial(fwd_kernel, step, group),
                grid_spec=pltpu.PrefetchScalarGridSpec(
                    num_scalar_prefetch=1,
                    grid=(grid,),
                    in_specs=[
                        pl.BlockSpec((step * seq, width), lambda i, s: (i, 0)),
                        pl.BlockSpec((width, 3 * gw), lambda i, s: (0, 0)),
                        pl.BlockSpec((group, seq, seq), lambda i, s, g=g: (g, 0, 0)),
                    ],
                    out_specs=[
                        pl.BlockSpec((step * seq, 3 * gw), lambda i, s: (i, 0)),
                        pl.BlockSpec((step, group, seq, seq), lambda i, s: (i, 0, 0, 0)),
                        pl.BlockSpec((step, group, seq), lambda i, s: (i, 0, 0)),
                        pl.BlockSpec((step, 1, gw), lambda i, s: (i, 0, 0)),
                    ],
                ),
                out_shape=[
                    struct((pairs * seq, 3 * gw), BF16),
                    struct((pairs, group, seq, seq), BF16),
                    struct((pairs, group, seq), F32),
                    struct((pairs, 1, gw), F32),
                ],
                name="fwd%d" % g,
            )(lens, normed, chunks[g], bias_t)
        )

    pooled, ctx, own = pl.pallas_call(
        functools.partial(score_kernel, groups),
        in_specs=[VM] * (groups + 5),
        out_specs=[VM] * 3,
        out_shape=[
            struct((pairs, width), F32),
            struct((pairs, width), F32),
            struct((pairs, LANES), F32),
        ],
        name="score",
    )(*[s[3].reshape(pairs, gw) for s in saved], mean.reshape(pairs, width), len_col, label_col, wo, sw)

    n_cand = lax.axis_size("cand")
    everyone = [own]
    for m in range(1, n_cand):
        everyone.append(lax.ppermute(own, "cand", [(i, i ^ m) for i in range(n_cand)]))
    everyone = jnp.concatenate(everyone, axis=0)

    a = pl.pallas_call(
        functools.partial(value_kernel, groups, group),
        grid=(pairs,),
        in_specs=[pl.BlockSpec((1, group, seq), lambda i: (i, 0, 0))] * groups
        + [pl.BlockSpec((seq, width), lambda i: (i, 0))],
        out_specs=pl.BlockSpec((1, heads, width), lambda i: (i, 0, 0)),
        out_shape=struct((pairs, heads, width), F32),
        name="value",
    )(*[s[2] for s in saved], normed)
    a = jnp.swapaxes(a, 0, 1).reshape(heads * pairs, width)

    g_all, dwo, dwv, loss = pl.pallas_call(
        functools.partial(head_kernel, c_local, heads),
        in_specs=[VM] * 7,
        out_specs=[VM] * 4,
        out_shape=[
            struct((pairs, width), BF16),
            struct((width, width), BF16),
            struct((width, width), BF16),
            struct((8, LANES), F32),
        ],
        name="head",
    )(everyone, pooled, ctx, len_col, a, wo, sw)
    loss = loss[0, :q_local]

    dqk = []
    for g in range(groups):
        dqk.append(
            pl.pallas_call(
                functools.partial(bwd_kernel, step, group),
                grid=(grid,),
                in_specs=[
                    pl.BlockSpec((step * seq, 3 * gw), lambda i: (i, 0)),
                    pl.BlockSpec((step, group, seq, seq), lambda i: (i, 0, 0, 0)),
                    pl.BlockSpec((step, 1, gw), lambda i, g=g: (i, 0, g)),
                    pl.BlockSpec((width, step * seq), lambda i: (0, i)),
                ],
                out_specs=pl.BlockSpec((width, 2 * gw), lambda i: (0, 0)),
                out_shape=struct((width, 2 * gw), BF16),
                scratch_shapes=[
                    pltpu.VMEM((width, 2 * gw), F32),
                    pltpu.VMEM((gw, step * seq), BF16),
                    pltpu.VMEM((step * seq, gw), BF16),
                ],
                name="bwd%d" % g,
            )(saved[g][0], saved[g][1], g_all.reshape(pairs, 1, width), normed_t)
        )
    partial = jnp.concatenate(
        [d[:, :gw] for d in dqk] + [d[:, gw:] for d in dqk] + [dwv, dwo], axis=1
    )
    shard = lax.psum_scatter(partial, "dp", scatter_dimension=0, tiled=True)
    shard = lax.psum(shard, "cand").astype(F32)
    squares = lax.psum(jnp.sum(shard * shard), "dp")
    update = shard / (jnp.sqrt(squares / (4.0 * width * width)) + EPS)
    return (update, loss)


def solution(mesh):
    in_specs = (
        P("dp", "cand", None, None),
        P("dp", None),
        P(),
        P(),
        P(),
        P("dp", "cand"),
        P("dp", "cand"),
    )
    out_specs = (P("dp", None), P("dp"))
    return jax.shard_map(shards, mesh=mesh, in_specs=in_specs, out_specs=out_specs, check_vma=False)
```

```python
import functools

import jax
import jax.numpy as jnp
from jax import lax
from jax.experimental import pallas as pl
from jax.experimental.pallas import tpu as pltpu
from jax.sharding import PartitionSpec as P

EPS = 1e-06
F32 = jnp.float32
BF16 = jnp.bfloat16
LANES = 128
COST = 100_000_000
NN = (((1,), (0,)), ((), ()))
NT = (((1,), (1,)), ((), ()))
TN = (((0,), (0,)), ((), ()))


def dot(a, b, dims=NN):
    return lax.dot_general(a, b, dims, preferred_element_type=F32)


def split2(x):
    high = x.astype(BF16)
    return high, (x - high.astype(F32)).astype(BF16)


def tree(parts):
    parts = list(parts)
    while len(parts) > 1:
        parts = [functools.reduce(jnp.add, parts[i : i + 2]) for i in range(0, len(parts), 2)]
    return parts[0]


def unpack(off_ref, piece_refs, wide_ref, w_ref):
    n = 0
    for ref in piece_refs:
        for i in range(ref.shape[0]):
            start = pl.multiple_of(off_ref[n], 8)
            wide_ref[pl.ds(start, ref.shape[1]), :] = ref[i].astype(F32)
            n += 1
    w_ref[...] = wide_ref[...].astype(BF16)


def pack(off_ref, wide_ref, piece_refs):
    n = 0
    for ref in piece_refs:
        for i in range(ref.shape[0]):
            start = pl.multiple_of(off_ref[n], 8)
            ref[i] = wide_ref[pl.ds(start, ref.shape[1]), :].astype(BF16)
            n += 1


def norm_kernel(step, len_ref, hid_ref, gain_ref, normed_ref, normed_t_ref, mean_ref):
    seq = hid_ref.shape[1]
    for b in range(step):
        pair_len = len_ref[pl.program_id(0) * step + b]
        x = hid_ref[b].astype(F32)
        factor = lax.rsqrt(jnp.mean(x * x, axis=-1, keepdims=True) + EPS)
        n = (x * factor * gain_ref[...]).astype(BF16)
        normed_ref[b * seq : (b + 1) * seq, :] = n
        normed_t_ref[:, b * seq : (b + 1) * seq] = n.T
        live = lax.broadcasted_iota(jnp.int32, x.shape, 0) < pair_len
        total = jnp.sum(jnp.where(live, x, 0.0), axis=0, keepdims=True)
        mean_ref[pl.ds(pl.program_id(0) * step + b, 1), :] = total / pair_len.astype(F32)


def fwd_kernel(step, heads, parts, len_ref, off_ref, normed_ref, bias_ref, *refs):
    piece_refs = refs[:parts]
    qkv_ref, pt_ref, c_ref, ctx_ref, wide_ref, w_ref = refs[parts:]

    @pl.when(pl.program_id(0) == 0)
    def _():
        unpack(off_ref, piece_refs, wide_ref, w_ref)

    seq = bias_ref.shape[1]
    width = w_ref.shape[1] // 3
    hd = width // heads
    qkv_ref[...] = dot(normed_ref[...], w_ref[...]).astype(BF16)
    ones = jnp.ones((8, seq), BF16)
    for b in range(step):
        pair_len = len_ref[pl.program_id(0) * step + b]
        rows = slice(b * seq, (b + 1) * seq)
        key_live = lax.broadcasted_iota(jnp.int32, (seq, seq), 0) < pair_len
        query_live = lax.broadcasted_iota(jnp.int32, (1, seq), 1) < pair_len
        sums = []
        for h in range(heads):
            q = qkv_ref[rows, h * hd : (h + 1) * hd]
            k = qkv_ref[rows, width + h * hd : width + (h + 1) * hd]
            st = dot(k, q, NT) + bias_ref[h]
            st = jnp.where(key_live, st, -1e30)
            e = jnp.exp(st - jnp.max(st, axis=0, keepdims=True))
            share = jnp.where(query_live, 1.0 / jnp.sum(e, axis=0, keepdims=True), 0.0)
            pt = (e * share).astype(BF16)
            pt_ref[b, h] = pt
            sums.append(dot(ones, pt, NT)[0:1, :])
        c = jnp.concatenate(sums, axis=0)
        c_ref[b] = c
        high, low = split2(c)
        v = qkv_ref[rows, 2 * width : 3 * width]
        ctx = dot(high, v) + dot(low, v)
        col_head = lax.broadcasted_iota(jnp.int32, ctx.shape, 1) // hd
        own = col_head == lax.broadcasted_iota(jnp.int32, ctx.shape, 0)
        row = pl.program_id(0) * step + b
        ctx_ref[pl.ds(row, 1), :] = jnp.sum(jnp.where(own, ctx, 0.0), axis=0, keepdims=True)


def value_kernel(step, groups, heads, rows, *refs):
    c_refs, (normed_ref, a_ref) = refs[:groups], refs[groups:]
    seq = c_refs[0].shape[2]
    for b in range(step):
        c = [r[b] for r in c_refs]
        if rows > groups * heads:
            c.append(jnp.zeros((rows - groups * heads, seq), F32))
        c = jnp.concatenate(c, axis=0).astype(BF16)
        a = dot(c, normed_ref[b * seq : (b + 1) * seq, :])
        a_ref[b * rows : (b + 1) * rows, :] = a.astype(BF16)


def score_kernel(groups, parts, off_ref, *refs):
    ctx_refs, refs = refs[:groups], refs[groups:]
    mean_ref, len_ref, label_ref, sw_ref = refs[:4]
    piece_refs, refs = refs[4 : 4 + parts], refs[4 + parts :]
    pooled_ref, ctx_ref, out_ref, wo_ref, wide_ref = refs
    unpack(off_ref, piece_refs, wide_ref, wo_ref)
    ctx = jnp.concatenate([r[...] for r in ctx_refs], axis=1)
    ctx_ref[...] = ctx
    high, low = split2(ctx / len_ref[...])
    pooled = mean_ref[...] + dot(high, wo_ref[...]) + dot(low, wo_ref[...])
    pooled_ref[...] = pooled
    factor = lax.rsqrt(jnp.mean(pooled * pooled, axis=-1, keepdims=True) + EPS)
    scores = jnp.sum(pooled * factor * sw_ref[...], axis=-1, keepdims=True)
    lane = lax.broadcasted_iota(jnp.int32, out_ref.shape, 1)
    out_ref[...] = jnp.where(lane == 0, scores, label_ref[...])


def head_kernel(c_local, heads, rows, parts, others, off_ref, *refs):
    all_refs, refs = refs[:others], refs[others:]
    pooled_ref, ctx_ref, len_ref, a_ref, wo_ref, sw_ref = refs[:6]
    g_ref, loss_ref = refs[6:8]
    wo_pieces, wv_pieces = refs[8 : 8 + parts], refs[8 + parts : 8 + 2 * parts]
    wide_o, wide_v = refs[8 + 2 * parts :]
    pairs, width = pooled_ref.shape
    hd = width // heads
    score = [r[:, 0:1] for r in all_refs]
    label = [r[:, 1:2] for r in all_refs]
    weight = [jnp.exp(x) for x in label]
    query = lax.broadcasted_iota(jnp.int32, score[0].shape, 0) // c_local
    score_grad = jnp.zeros_like(score[0])
    lane = lax.broadcasted_iota(jnp.int32, loss_ref.shape, 1)
    losses = jnp.zeros(loss_ref.shape, F32)

    def total(mine, parts):
        return tree(jnp.sum(jnp.where(mine, x, 0.0), axis=0, keepdims=True) for x in parts)

    for q in range(pairs // c_local):
        mine = query == q
        tops = [jnp.max(jnp.where(mine, x, -jnp.inf), axis=0, keepdims=True) for x in score]
        highest = functools.reduce(jnp.maximum, tops)
        expsum = total(mine, [jnp.exp(x - highest) for x in score])
        tsum = total(mine, weight)
        tdot = total(mine, [w * x for w, x in zip(weight, score)])
        losses = jnp.where(lane == q, highest + jnp.log(expsum) - tdot / tsum, losses)
        grad = jnp.exp(score[0] - highest) / expsum - weight[0] / tsum
        score_grad = jnp.where(mine, grad, score_grad)
    loss_ref[...] = losses
    pooled = pooled_ref[...]
    sw = sw_ref[...]
    factor = lax.rsqrt(jnp.mean(pooled * pooled, axis=-1, keepdims=True) + EPS)
    inner = jnp.sum(pooled * sw, axis=-1, keepdims=True) / width
    pooled_grad = score_grad * (factor * sw - pooled * (factor * factor * factor * inner))
    out_grad = (pooled_grad / len_ref[...]).astype(BF16)
    high, low = split2(ctx_ref[...])
    wide_o[...] = dot(
        jnp.concatenate([high, low], axis=0), jnp.concatenate([out_grad, out_grad], axis=0), TN
    )
    pack(off_ref, wide_o, wo_pieces)
    g = dot(out_grad, wo_ref[...], NT).astype(BF16).astype(F32)
    g_ref[...] = g
    col_head = lax.broadcasted_iota(jnp.int32, (rows, width), 1) // hd
    own = col_head == lax.broadcasted_iota(jnp.int32, (rows, width), 0)
    spread = [jnp.where(own, g[p : p + 1, :], 0.0).astype(BF16) for p in range(pairs)]
    wide_v[...] = dot(a_ref[...], jnp.concatenate(spread, axis=0), TN)
    pack(off_ref, wide_v, wv_pieces)


def bwd_kernel(step, heads, parts, off_ref, qkv_ref, pt_ref, g_ref, nt_ref, *refs):
    piece_refs = refs[:parts]
    acc_ref, dqt_ref, dk_ref = refs[parts:]
    seq = pt_ref.shape[2]
    width = qkv_ref.shape[1] // 3
    hd = width // heads
    for b in range(step):
        rows = slice(b * seq, (b + 1) * seq)
        kt = qkv_ref[rows, width : 2 * width].T
        g = g_ref[pl.ds(pl.program_id(0) * step + b, 1), :].astype(BF16)
        for h in range(heads):
            cols = slice(h * hd, (h + 1) * hd)
            v = qkv_ref[rows, 2 * width + h * hd : 2 * width + (h + 1) * hd]
            u = dot(v, jnp.broadcast_to(g[:, cols], (seq, hd)), NT)
            pt = pt_ref[b, h].astype(F32)
            r = jnp.sum(pt * u, axis=0, keepdims=True)
            t = (pt * (u - r)).astype(BF16)
            dk_ref[rows, cols] = dot(t, qkv_ref[rows, cols]).astype(BF16)
            dqt_ref[cols, rows] = dot(kt[cols, :], t).astype(BF16)

    @pl.when(pl.program_id(0) == 0)
    def _():
        acc_ref[...] = jnp.zeros_like(acc_ref)

    acc_ref[:, :width] += dot(nt_ref[...], dqt_ref[...], NT)
    acc_ref[:, width:] += dot(nt_ref[...], dk_ref[...])

    @pl.when(pl.program_id(0) == pl.num_programs(0) - 1)
    def _():
        pack(off_ref, acc_ref, piece_refs)


def final_kernel(spans, n_cand, n_sq, off_ref, *refs):
    sq_refs, refs = refs[:n_sq], refs[n_sq:]
    piece_refs, out_ref = refs[:-1], refs[-1]
    width = out_ref.shape[1] // 4
    squares = tree(r[0:1, 0:1] for r in sq_refs)
    scale = 1.0 / (jnp.sqrt(squares / (4.0 * width * width)) + EPS)
    n = 0
    for span in spans:
        for m in range(n_cand):
            ref = piece_refs[n]
            n += 1
            rows = pl.ds(pl.multiple_of(off_ref[m], 8), ref.shape[0])
            start = 0
            for col, size in span:
                out_ref[rows, col : col + size] = ref[:, start : start + size].astype(F32) * scale
                start += size


VM = pl.BlockSpec(memory_space=pltpu.VMEM)


def struct(shape, dtype):
    return jax.ShapeDtypeStruct(shape, dtype)


def swap(x, axis, mask):
    n = lax.axis_size(axis)
    return lax.ppermute(x, axis, [(i, i ^ mask) for i in range(n)])


def relative(stages):
    rel = [(0, 0)]
    for axis, masks in stages:
        steps = [(m, 0) if axis == "dp" else (0, m) for m in (0, *masks)]
        rel = [(d ^ e, c ^ f) for e, f in steps for d, c in rel]
    return rel


def gather(piece, stages):
    stack = piece[None]
    for n, (axis, masks) in enumerate(stages):
        parts = [stack] + [swap(stack, axis, m) for m in masks]
        if n == len(stages) - 1:
            return parts
        stack = jnp.concatenate(parts, axis=0)


def reduce(parts, stages):
    for n, (axis, masks) in enumerate(stages):
        if n:
            size = parts[0].shape[0] // (1 + len(masks))
            parts = [
                tree(p[i * size : (i + 1) * size].astype(F32) for p in parts).astype(BF16)
                for i in range(1 + len(masks))
            ]
        parts = [parts[0]] + [swap(p, axis, m) for p, m in zip(parts[1:], masks)]
    return tree(p[0].astype(F32) for p in parts)


def shards(hidden, attn_weight, norm_gain, pos_bias, score_weight, pair_lengths, labels):
    q_local, c_local, seq, width = hidden.shape
    heads = pos_bias.shape[0]
    hd = width // heads
    pairs = q_local * c_local
    group = max(1, min(heads, 256 // hd))
    while heads % group:
        group -= 1
    groups = heads // group
    gw = group * hd
    step = 4
    while pairs % step:
        step //= 2
    grid = pairs // step
    a_rows = -(-heads // 16) * 16
    n_dp, n_cand = lax.axis_size("dp"), lax.axis_size("cand")
    own_rows = attn_weight.shape[0]
    rows = own_rows // n_cand
    staged = rows % 8 == 0 and n_dp & (n_dp - 1) == 0 and n_cand & (n_cand - 1) == 0

    tokens = hidden.reshape(pairs, seq, width)
    lens = pair_lengths.reshape(-1)
    len_col = lens.astype(F32)[:, None]
    label_col = labels.reshape(-1).astype(F32)[:, None]
    bias_t = jnp.swapaxes(pos_bias, 1, 2)
    sw = score_weight[None, :]

    far = ("dp", tuple(range(2, n_dp, 2)))
    near = ("dp", (1,))
    across = ("cand", tuple(range(2, n_cand, 2)))
    core = ("cand", (1,))
    orders = [[far, near, across, core], [far, across, near, core]]
    me_dp, me_cand = lax.axis_index("dp"), lax.axis_index("cand")

    def offsets(rel):
        d = jnp.array([r[0] for r in rel], jnp.int32)
        c = jnp.array([r[1] for r in rel], jnp.int32)
        return ((me_dp ^ d) * n_cand + (me_cand ^ c)) * rows

    def columns(x, g):
        if g == groups:
            return x[:, 3 * width :]
        return jnp.concatenate(
            [x[:, s * width + g * gw : s * width + (g + 1) * gw] for s in range(3)], axis=1
        )

    if staged:
        mine = lax.dynamic_slice_in_dim(attn_weight, me_cand * rows, rows, axis=0)
        chunks = [gather(columns(mine, g), orders[g % 2]) for g in range(groups + 1)]
        offs = [offsets(relative(orders[g % 2])) for g in range(2)]
        back = [list(reversed(o)) for o in orders]
        r_offs = [offs[0], offs[1]]
        half = n_dp * n_cand // 2
        out_parts = [(half, rows), (half, rows)]
    else:
        weights = lax.all_gather(attn_weight, "dp", axis=0, tiled=True)
        chunks = [[columns(weights, g)[None]] for g in range(groups + 1)]
        offs = [jnp.zeros((1,), jnp.int32)] * 2
        r_offs = offs
        out_parts = [(1, width)]

    def pieces(cols):
        return [struct((n, r, cols), BF16) for n, r in out_parts]

    normed, normed_t, mean = pl.pallas_call(
        functools.partial(norm_kernel, step),
        grid_spec=pltpu.PrefetchScalarGridSpec(
            num_scalar_prefetch=1,
            grid=(grid,),
            in_specs=[
                pl.BlockSpec((step, seq, width), lambda i, s: (i, 0, 0)),
                pl.BlockSpec((1, width), lambda i, s: (0, 0)),
            ],
            out_specs=[
                pl.BlockSpec((step * seq, width), lambda i, s: (i, 0)),
                pl.BlockSpec((width, step * seq), lambda i, s: (0, i)),
                pl.BlockSpec((pairs, width), lambda i, s: (0, 0)),
            ],
        ),
        out_shape=[
            struct((pairs * seq, width), BF16),
            struct((width, pairs * seq), BF16),
            struct((pairs, width), F32),
        ],
        cost_estimate=pl.CostEstimate(flops=COST * 6, transcendentals=0, bytes_accessed=0),
        name="norm",
    )(lens, tokens, norm_gain[None, :])

    saved = []
    for g in range(groups):
        chunk = chunks[g]
        saved.append(
            pl.pallas_call(
                functools.partial(fwd_kernel, step, group, len(chunk)),
                grid_spec=pltpu.PrefetchScalarGridSpec(
                    num_scalar_prefetch=2,
                    grid=(grid,),
                    in_specs=[
                        pl.BlockSpec((step * seq, width), lambda i, s, o: (i, 0)),
                        pl.BlockSpec((group, seq, seq), lambda i, s, o, g=g: (g, 0, 0)),
                    ]
                    + [pl.BlockSpec(p.shape, lambda i, s, o: (0, 0, 0)) for p in chunk],
                    out_specs=[
                        pl.BlockSpec((step * seq, 3 * gw), lambda i, s, o: (i, 0)),
                        pl.BlockSpec((step, group, seq, seq), lambda i, s, o: (i, 0, 0, 0)),
                        pl.BlockSpec((step, group, seq), lambda i, s, o: (i, 0, 0)),
                        pl.BlockSpec((pairs, gw), lambda i, s, o: (0, 0)),
                    ],
                    scratch_shapes=[
                        pltpu.VMEM((width, 3 * gw), F32),
                        pltpu.VMEM((width, 3 * gw), BF16),
                    ],
                ),
                out_shape=[
                    struct((pairs * seq, 3 * gw), BF16),
                    struct((pairs, group, seq, seq), BF16),
                    struct((pairs, group, seq), F32),
                    struct((pairs, gw), F32),
                ],
                cost_estimate=pl.CostEstimate(flops=COST * 14, transcendentals=0, bytes_accessed=0),
                name="fwd%d" % g,
            )(lens, offs[g % 2], normed, bias_t, *chunk)
        )

    chunk = chunks[groups]
    smem = pl.BlockSpec(memory_space=pltpu.SMEM)
    pooled, ctx, own, wo = pl.pallas_call(
        functools.partial(score_kernel, groups, len(chunk)),
        in_specs=[smem] + [VM] * (groups + 4 + len(chunk)),
        out_specs=[VM] * 4,
        out_shape=[
            struct((pairs, width), F32),
            struct((pairs, width), F32),
            struct((pairs, LANES), F32),
            struct((width, width), BF16),
        ],
        scratch_shapes=[pltpu.VMEM((width, width), F32)],
        cost_estimate=pl.CostEstimate(flops=COST * 3, transcendentals=0, bytes_accessed=0),
        name="score",
    )(offs[groups % 2], *[s[3] for s in saved], mean, len_col, label_col, sw, *chunk)

    if n_cand & (n_cand - 1) == 0:
        everyone = [own] + [swap(own, "cand", m) for m in range(1, n_cand)]
    else:
        everyone = list(lax.all_gather(own, "cand"))

    a = pl.pallas_call(
        functools.partial(value_kernel, step, groups, group, a_rows),
        grid=(grid,),
        in_specs=[pl.BlockSpec((step, group, seq), lambda i: (i, 0, 0))] * groups
        + [pl.BlockSpec((step * seq, width), lambda i: (i, 0))],
        out_specs=pl.BlockSpec((step * a_rows, width), lambda i: (i, 0)),
        out_shape=struct((pairs * a_rows, width), BF16),
        cost_estimate=pl.CostEstimate(flops=COST * 4, transcendentals=0, bytes_accessed=0),
        name="value",
    )(*[s[2] for s in saved], normed)

    n_parts = len(out_parts)
    g_all, loss, *dvo = pl.pallas_call(
        functools.partial(head_kernel, c_local, heads, a_rows, n_parts, n_cand),
        in_specs=[smem] + [VM] * (n_cand + 6),
        out_specs=[VM] * (2 + 2 * n_parts),
        out_shape=[struct((pairs, width), F32), struct((8, LANES), F32)]
        + pieces(width) * 2,
        scratch_shapes=[pltpu.VMEM((width, width), F32)] * 2,
        cost_estimate=pl.CostEstimate(flops=COST * 4, transcendentals=0, bytes_accessed=0),
        name="head",
    )(r_offs[0], *everyone, pooled, ctx, len_col, a, wo, sw)
    loss = loss[0, :q_local]
    grads = [dvo[:n_parts], dvo[n_parts:]]
    spans = [[(3 * width, width)], [(2 * width, width)]]

    for g in range(groups):
        grads.append(
            pl.pallas_call(
                functools.partial(bwd_kernel, step, group, n_parts),
                grid_spec=pltpu.PrefetchScalarGridSpec(
                    num_scalar_prefetch=1,
                    grid=(grid,),
                    in_specs=[
                        pl.BlockSpec((step * seq, 3 * gw), lambda i, o: (i, 0)),
                        pl.BlockSpec((step, group, seq, seq), lambda i, o: (i, 0, 0, 0)),
                        pl.BlockSpec((pairs, gw), lambda i, o, g=g: (0, g)),
                        pl.BlockSpec((width, step * seq), lambda i, o: (0, i)),
                    ],
                    out_specs=[
                        pl.BlockSpec(p.shape, lambda i, o: (0, 0, 0)) for p in pieces(2 * gw)
                    ],
                    scratch_shapes=[
                        pltpu.VMEM((width, 2 * gw), F32),
                        pltpu.VMEM((gw, step * seq), BF16),
                        pltpu.VMEM((step * seq, gw), BF16),
                    ],
                ),
                out_shape=pieces(2 * gw),
                cost_estimate=pl.CostEstimate(flops=COST * 9, transcendentals=0, bytes_accessed=0),
                name="bwd%d" % g,
            )(r_offs[g % 2], saved[g][0], saved[g][1], g_all, normed_t)
        )
        spans.append([(g * gw, gw), (width + g * gw, gw)])

    if not staged:
        flat = [g[0][0] for g in grads]
        partial = jnp.concatenate(
            [d[:, :gw] for d in flat[2:]] + [d[:, gw:] for d in flat[2:]] + [flat[1], flat[0]],
            axis=1,
        )
        shard = lax.psum_scatter(partial, "dp", scatter_dimension=0, tiled=True)
        shard = lax.psum(shard, "cand").astype(F32)
        squares = lax.psum(jnp.sum(shard * shard), "dp")
        update = shard / (jnp.sqrt(squares / (4.0 * width * width)) + EPS)
        return (update, loss)

    which = [0, 0] + [g % 2 for g in range(groups)]
    done = [reduce(p, back[w]).astype(BF16) for p, w in zip(grads, which)]
    squares = tree(jnp.sum(jnp.square(d.astype(F32))) for d in done)
    squares = jnp.broadcast_to(squares, (8, LANES))
    squares = tree([squares] + [swap(squares, "cand", m) for m in range(1, n_cand)])
    squares = [squares] + [swap(squares, "dp", m) for m in range(1, n_dp)]
    final = []
    for d in done:
        final += [d] + [swap(d, "cand", m) for m in range(1, n_cand)]
    row_offs = (me_cand ^ jnp.arange(n_cand, dtype=jnp.int32)) * rows
    update = pl.pallas_call(
        functools.partial(final_kernel, spans, n_cand, n_dp),
        in_specs=[smem] + [VM] * (n_dp + len(final)),
        out_specs=VM,
        out_shape=struct((own_rows, 4 * width), F32),
        name="final",
    )(row_offs, *squares, *final)
    return (update, loss)


def solution(mesh):
    in_specs = (
        P("dp", "cand", None, None),
        P("dp", None),
        P(),
        P(),
        P(),
        P("dp", "cand"),
        P("dp", "cand"),
    )
    out_specs = (P("dp", None), P("dp"))
    return jax.shard_map(shards, mesh=mesh, in_specs=in_specs, out_specs=out_specs, check_vma=False)
```
